32 devices in a mesh: seq: 4 (over z), head: 4 (over y, core), batch: 2 (over x).
Axes of the slice: x: 2, y: 2, z: 4, core: 2. Of those that a mesh axis runs over, the one named last changes fastest.
Arguments:
- tokens: bfloat16 [8192, 2048], P(('batch', 'seq')), parts along dimension 0, may hold values from -6 to 6
- neighbor_bank: bfloat16 [128, 256, 2048], P(('batch', 'seq')), parts along dimension 0, may hold values from -2100 to 2100
- slots: int32 [128], P(('batch', 'seq')), parts along dimension 0, may hold values from 0 to 15
- w_query: bfloat16 [2048, 2048], P('seq', 'head'), may hold values from -0.125 to 0.125
- w_key: bfloat16 [2048, 2048], P('seq', 'head'), may hold values from -0.125 to 0.125
- w_value: bfloat16 [2048, 2048], P('seq', 'head'), may hold values from -0.125 to 0.125
- w_out: bfloat16 [2048, 2048], P('head', 'seq'), may hold values from -0.125 to 0.125
Outputs:
- cross_out: bfloat16 [8192, 2048], P(('batch', 'seq'), 'head'), parts along dimension 0
The draws below stay inside these ranges and needn't reach their ends.
There are 2 independent parts, one for each index of `batch`. The reference program is written for one: setup_inputs(seed, part) draws one part's arguments, and reference() takes and returns one part's arrays. A program takes and returns all parts, laid end to end along the dimension named above; an argument that names none is the same for every part. Nothing has to cross between parts.
Inputs may be any that keep to these rules, and one draw needn't show every extreme that they name: Entry c picks row c // 16 * 16 + slots[c] of neighbor_bank.
All inputs are finite; a program needn't handle non-finite values.
Results may differ from the reference program's by a relative error of at most 0.006.
The reference program's roundings to bfloat16 on the way (of `normed`, `queries`, `retrieved`, `weights` and `attended`) count: a program that leaves them out, or rounds other values in their place, can miss the bound.
Values may be sent and summed in bfloat16 or wider, within the bound.
No kernel may reach another device: no remote copies, remote signals or barrier semaphores. Data moves between devices by JAX's collectives and lax.ppermute only.
A program may use at most 128 MiB of HBM per device.

```python
import math
import jax
import jax.numpy as jnp
from jax import lax

D = 2048
HEADS = 16
HEAD_DIM = 128
BLOCK = 64
NEIGHBORS = 2
NEIGH_LEN = 128
BLOCK_DEV = 16
TOKENS = 4096
BLOCKS = 64


def draw_neighbor_bank(key, part):
    key_base = jax.random.fold_in(jax.random.fold_in(key, 11), 0)
    rows = NEIGHBORS * NEIGH_LEN
    base = jnp.clip(jax.random.normal(key_base, (BLOCKS, rows, D), jnp.float32) * 2.0, -8.0, 8.0)
    return base.astype(jnp.bfloat16)


def plant(drawn, own_key, low, largest):
    dims = drawn.shape
    spot = [jax.random.randint(jax.random.fold_in(own_key, axis), (), 0, dims[axis]) for axis in range(len(dims))]
    drawn = drawn.at[tuple(spot)].set(low)
    longest = dims.index(max(dims))
    spot[longest] = (spot[longest] + 1) % dims[longest]
    return drawn.at[tuple(spot)].set(largest)


def block_scale(rng, extent, cuts, smallest, high):
    def one(dim, parts):
        steps = jax.random.uniform(jax.random.fold_in(jax.random.fold_in(rng, 6), dim), (parts,), jnp.float32, smallest / len(cuts), high / len(cuts))
        return jnp.repeat(jnp.exp(steps), extent[dim] // parts).reshape((-1,) + (1,) * (len(extent) - dim - 1))

    loudness = one(*cuts[0])
    for cut in cuts[1:]:
        loudness = loudness * one(*cut)
    return loudness


def noise(key, dims, scale, reach, cuts=(), kind=jnp.bfloat16):
    entries = jax.random.normal(key, dims, jnp.float32) * scale
    if len(cuts) > 0:
        entries = block_scale(key, dims, cuts, -0.22, 0.18) * entries
    return jnp.clip(entries, min=-reach, max=reach).astype(kind)


def setup_inputs(seed: int = 0, part: int = 0) -> dict:
    streams_of = jax.random.split(jax.random.key(seed), 8)
    part_splits = jax.random.split(jax.random.fold_in(streams_of[7], part), 8)
    tokens = noise(part_splits[0], (TOKENS, D), 1.0, 6.0, ((0, 4),))
    neighbor_bank = draw_neighbor_bank(jax.random.fold_in(jax.random.fold_in(streams_of[7], part), 71), part)
    slots = plant(jax.random.randint(part_splits[2], (BLOCKS,), 0, BLOCK_DEV), jax.random.fold_in(part_splits[2], 1), 0, BLOCK_DEV - 1).astype(jnp.int32)
    w_query = noise(streams_of[3], (D, D), D ** -0.5, 0.125, ((0, 4), (1, 4)))
    w_key = noise(streams_of[4], (D, D), D ** -0.5, 0.125, ((0, 4), (1, 4)))
    w_value = noise(streams_of[5], (D, D), D ** -0.5, 0.125, ((0, 4), (1, 4)))
    w_out = noise(streams_of[6], (D, D), D ** -0.5, 0.125, ((0, 4), (1, 4)))
    return {"tokens": tokens, "neighbor_bank": neighbor_bank, "slots": slots, "w_query": w_query, "w_key": w_key, "w_value": w_value, "w_out": w_out}


def rms_normed(tokens):
    hidden = tokens.astype(jnp.float32)
    scale_row = lax.rsqrt(lax.optimization_barrier(jnp.mean(hidden * hidden, axis=-1, keepdims=True)) + 1e-06)
    return (hidden * scale_row).astype(jnp.bfloat16)

def reference(tokens, neighbor_bank, slots, w_query, w_key, w_value, w_out):
    normed = rms_normed(tokens)
    queries = jnp.dot(normed, w_query, preferred_element_type=jnp.float32).astype(jnp.bfloat16)
    block_ids = jnp.arange(BLOCKS, dtype=jnp.int32)
    bank_rows = (block_ids // BLOCK_DEV * BLOCK_DEV + slots).astype(jnp.int32)
    retrieved = jnp.take(neighbor_bank, bank_rows, axis=0).reshape(BLOCKS * NEIGHBORS * NEIGH_LEN, D)
    key_rows = jnp.dot(retrieved, w_key, preferred_element_type=jnp.float32).astype(jnp.bfloat16)
    value_rows = jnp.dot(retrieved, w_value, preferred_element_type=jnp.float32).astype(jnp.bfloat16)
    key_rows = key_rows.reshape(BLOCKS, NEIGHBORS * NEIGH_LEN, HEADS, HEAD_DIM)
    value_rows = value_rows.reshape(BLOCKS, NEIGHBORS * NEIGH_LEN, HEADS, HEAD_DIM)
    padding = jnp.zeros((1, NEIGHBORS * NEIGH_LEN, HEADS, HEAD_DIM), jnp.bfloat16)
    prior_keys = jnp.concatenate([padding, key_rows[:-1]], axis=0)
    prior_values = jnp.concatenate([padding, value_rows[:-1]], axis=0)
    query_blocks = queries.reshape(BLOCKS, BLOCK, HEADS, HEAD_DIM)
    scores = jnp.einsum('cmhd,cnhd->chmn', query_blocks.astype(jnp.float32), prior_keys.astype(jnp.float32)) / math.sqrt(HEAD_DIM)
    peak_score = lax.optimization_barrier(jnp.max(scores, axis=-1, keepdims=True))
    exponent = jnp.exp(scores - peak_score)
    weights = (exponent / lax.optimization_barrier(jnp.sum(exponent, axis=-1, keepdims=True))).astype(jnp.bfloat16)
    attended = jnp.einsum('chmn,cnhd->cmhd', weights.astype(jnp.float32), prior_values.astype(jnp.float32))
    attended = attended.astype(jnp.bfloat16).reshape(TOKENS, D)
    return jnp.dot(attended, w_out, preferred_element_type=jnp.float32).astype(jnp.bfloat16)
```

```python
import math

import jax
import jax.numpy as jnp
from jax import lax
from jax.experimental import pallas as pl
from jax.experimental.pallas import tpu as pltpu
from jax.sharding import PartitionSpec as P

HEAD_DIM = 128
GROUPS = 2


def rotated(block, axis, distance):
    n = lax.axis_size(axis)
    return lax.ppermute(block, axis, [(i, (i + distance) % n) for i in range(n)])


def shifted(block, axis, distance):
    devices = range(lax.axis_size(axis))
    route = [(i, i + distance) for i in devices if i + distance in devices]
    return lax.ppermute(block, axis, route)


def ring(shard):
    n, copies = lax.axis_size("seq"), lax.axis_size("batch")
    me, copy = lax.axis_index("seq"), lax.axis_index("batch")
    rows = shard.shape[0]
    if n == 1:
        return [(shard, jnp.int32(0))]
    if rows % (copies * 16):
        copies, copy = 1, 0
    part = rows // copies
    ahead = n // 2
    pieces = [(shard, me * rows)]
    up = lax.dynamic_slice_in_dim(shard, copy * part, part, 0) if copies > 1 else shard
    down = shard
    for step in range(1, ahead + 1):
        up = rotated(up, "seq", 1)
        home = (me - step) % n * rows
        for turn in range(copies):
            other = rotated(up, "batch", turn) if turn else up
            pieces.append((other, home + (copy - turn) % copies * part))
        if step <= n - 1 - ahead:
            down = rotated(down, "seq", -1)
            pieces.append((down, (me + step) % n * rows))
    return pieces


def offsets_of(pieces):
    return jnp.stack([jnp.asarray(first, jnp.int32) for _, first in pieces])


def lay_out(firsts, pieces, whole):
    for k, piece in enumerate(pieces):
        rows = piece.shape[0]
        whole[pl.ds(pl.multiple_of(firsts[k], math.gcd(rows, 256)), rows), :] = piece[...]


def project(source, pieces, name, block=512):
    rows, depth = source.shape
    width = pieces[0][0].shape[1]
    block = math.gcd(rows, block)
    count = len(pieces)

    def body(firsts, source_ref, *refs):
        out_ref, whole = refs[count], refs[count + 1]

        @pl.when(pl.program_id(0) == 0)
        def _():
            lay_out(firsts, refs[:count], whole)

        out_ref[...] = jnp.dot(
            source_ref[...], whole[...], preferred_element_type=jnp.float32
        ).astype(jnp.bfloat16)

    return pl.pallas_call(
        body,
        grid_spec=pltpu.PrefetchScalarGridSpec(
            num_scalar_prefetch=1,
            grid=(rows // block,),
            in_specs=[pl.BlockSpec((block, depth), lambda i, _: (i, 0))]
            + [pl.BlockSpec(p.shape, lambda i, _: (0, 0)) for p, _ in pieces],
            out_specs=pl.BlockSpec((block, width), lambda i, _: (i, 0)),
            scratch_shapes=[pltpu.VMEM((depth, width), jnp.bfloat16)],
        ),
        out_shape=jax.ShapeDtypeStruct((rows, width), jnp.bfloat16),
        cost_estimate=pl.CostEstimate(
            flops=2 * rows * depth * width,
            bytes_accessed=2 * (rows * depth + depth * width + rows * width),
            transcendentals=0,
        ),
        name=name,
    )(offsets_of(pieces), source, *[p for p, _ in pieces])


def project_normed(tokens, pieces, name, block=256):
    rows, depth = tokens.shape
    width = pieces[0][0].shape[1]
    block = math.gcd(rows, block)
    count = len(pieces)

    def body(firsts, source_ref, *refs):
        out_ref, whole = refs[count], refs[count + 1]

        @pl.when(pl.program_id(0) == 0)
        def _():
            lay_out(firsts, refs[:count], whole)

        hidden = source_ref[...].astype(jnp.float32)
        scale = lax.rsqrt(jnp.mean(hidden * hidden, axis=-1, keepdims=True) + 1e-06)
        normed = (hidden * scale).astype(jnp.bfloat16)
        out_ref[...] = jnp.dot(normed, whole[...], preferred_element_type=jnp.float32).astype(
            jnp.bfloat16
        )

    return pl.pallas_call(
        body,
        grid_spec=pltpu.PrefetchScalarGridSpec(
            num_scalar_prefetch=1,
            grid=(rows // block,),
            in_specs=[pl.BlockSpec((block, depth), lambda i, _: (i, 0))]
            + [pl.BlockSpec(p.shape, lambda i, _: (0, 0)) for p, _ in pieces],
            out_specs=pl.BlockSpec((block, width), lambda i, _: (i, 0)),
            scratch_shapes=[pltpu.VMEM((depth, width), jnp.bfloat16)],
        ),
        out_shape=jax.ShapeDtypeStruct((rows, width), jnp.bfloat16),
        cost_estimate=pl.CostEstimate(
            flops=2 * rows * depth * width,
            bytes_accessed=2 * (rows * depth + depth * width + rows * width),
            transcendentals=0,
        ),
        name=name,
    )(offsets_of(pieces), tokens, *[p for p, _ in pieces])


def attend(queries, next_queries, key_value, slots, first_head, heads, name):
    blocks = slots.shape[0]
    block_len = queries.shape[0] // blocks
    neighbor_rows = key_value.shape[0] // blocks
    width = heads * HEAD_DIM
    lead = first_head * HEAD_DIM
    at_once = math.gcd(blocks, 4)
    root = 1.0 / math.sqrt(HEAD_DIM)

    def body(slot_ref, query_ref, next_ref, *refs):
        out_ref = refs[at_once]
        step = pl.program_id(0)
        for t in range(at_once):
            j = step * at_once + t
            begin = jnp.minimum(j + 1, blocks - 1) * block_len
            q_block = query_ref[pl.ds(pl.multiple_of(begin, block_len), block_len), lead : lead + width]
            if t == at_once - 1:
                q_block = jnp.where(j == blocks - 1, next_ref[:, lead : lead + width], q_block)
            for h in range(heads):
                col = h * HEAD_DIM
                q = q_block[:, col : col + HEAD_DIM]
                k = refs[t][:, col : col + HEAD_DIM]
                v = refs[t][:, width + col : width + col + HEAD_DIM]
                scores = (
                    lax.dot_general(
                        q, k, (((1,), (1,)), ((), ())), preferred_element_type=jnp.float32
                    )
                    * root
                )
                exponent = jnp.exp(scores - jnp.max(scores, axis=-1, keepdims=True))
                total = jnp.sum(exponent, axis=-1, keepdims=True)
                weights = (exponent / total).astype(jnp.bfloat16)
                out_ref[t * block_len : (t + 1) * block_len, col : col + HEAD_DIM] = jnp.dot(
                    weights, v, preferred_element_type=jnp.float32
                ).astype(jnp.bfloat16)

    def picked(t):
        return lambda i, slot_ref: (slot_ref[i * at_once + t], 0)

    return pl.pallas_call(
        body,
        grid_spec=pltpu.PrefetchScalarGridSpec(
            num_scalar_prefetch=1,
            grid=(blocks // at_once,),
            in_specs=[
                pl.BlockSpec(queries.shape, lambda i, _: (0, 0)),
                pl.BlockSpec(next_queries.shape, lambda i, _: (0, 0)),
            ]
            + [pl.BlockSpec((neighbor_rows, 2 * width), picked(t)) for t in range(at_once)],
            out_specs=pl.BlockSpec((at_once * block_len, width), lambda i, _: (i, 0)),
        ),
        out_shape=jax.ShapeDtypeStruct((blocks * block_len, width), jnp.bfloat16),
        cost_estimate=pl.CostEstimate(
            flops=4 * blocks * block_len * neighbor_rows * width * 4,
            bytes_accessed=2 * 2 * key_value.size,
            transcendentals=blocks * block_len * neighbor_rows * heads,
        ),
        name=name,
    )(slots, queries, next_queries, *[key_value] * at_once)


def every_head(own):
    n, me = lax.axis_size("head"), lax.axis_index("head")
    held = [own]
    if n & (n - 1):
        return [(own, me)] + [(rotated(own, "head", r), (me - r) % n) for r in range(1, n)]
    for r in range(1, n):
        bit = r & -r
        held.append(lax.ppermute(held[r ^ bit], "head", [(i, i ^ bit) for i in range(n)]))
    return [(piece, me ^ r) for r, piece in enumerate(held)]


def combine(parts, pieces, name, block=256):
    rows = parts[0][0].shape[0]
    width = pieces[0][0].shape[1]
    depth = sum(p.shape[0] for p, _ in pieces)
    block = math.gcd(rows, block)
    count, n_parts = len(pieces), len(parts)

    def body(firsts, starts, *refs):
        part_refs, piece_refs = refs[:n_parts], refs[n_parts : n_parts + count]
        out_ref, whole = refs[n_parts + count :]

        @pl.when(pl.program_id(0) == 0)
        def _():
            lay_out(firsts, piece_refs, whole)

        total = None
        for k, part in enumerate(part_refs):
            deep = part.shape[1]
            rows_k = whole[pl.ds(pl.multiple_of(starts[k], math.gcd(deep, 256)), deep), :]
            term = jnp.dot(part[...], rows_k, preferred_element_type=jnp.float32)
            total = term if total is None else total + term
        out_ref[...] = total.astype(jnp.bfloat16)

    return pl.pallas_call(
        body,
        grid_spec=pltpu.PrefetchScalarGridSpec(
            num_scalar_prefetch=2,
            grid=(rows // block,),
            in_specs=[pl.BlockSpec((block, a.shape[1]), lambda i, *_: (i, 0)) for a, _ in parts]
            + [pl.BlockSpec(p.shape, lambda i, *_: (0, 0)) for p, _ in pieces],
            out_specs=pl.BlockSpec((block, width), lambda i, *_: (i, 0)),
            scratch_shapes=[pltpu.VMEM((depth, width), jnp.bfloat16)],
        ),
        out_shape=jax.ShapeDtypeStruct((rows, width), jnp.bfloat16),
        cost_estimate=pl.CostEstimate(
            flops=2 * rows * depth * width,
            bytes_accessed=2 * (rows * depth + depth * width + rows * width),
            transcendentals=0,
        ),
        name=name,
    )(offsets_of(pieces), offsets_of(parts), *[a for a, _ in parts], *[p for p, _ in pieces])


def out_pieces(w_out):
    n_seq, n_head = lax.axis_size("seq"), lax.axis_size("head")
    if n_seq == n_head:
        route = [(s * n_head + h, h * n_head + s) for s in range(n_seq) for h in range(n_head)]
        return ring(lax.ppermute(w_out, ("seq", "head"), route))
    wide_rows = lax.all_gather(w_out, "seq", axis=1, tiled=True)
    own = lax.all_to_all(wide_rows, "head", split_axis=1, concat_axis=0, tiled=True)
    return [(own, jnp.int32(0))]


def local(tokens, neighbor_bank, slots, w_query, w_key, w_value, w_out):
    tok_rows, model_width = tokens.shape
    block_count, neighbor_rows, _ = neighbor_bank.shape
    block_len = tok_rows // block_count
    local_width = w_query.shape[1]
    local_heads = local_width // HEAD_DIM
    groups = math.gcd(local_heads, GROUPS)
    heads = local_heads // groups
    span = heads * HEAD_DIM
    bank = neighbor_bank.reshape(block_count * neighbor_rows, model_width)

    query_pieces = ring(w_query)
    group_pieces = []
    for g in range(groups):
        cut = slice(g * span, (g + 1) * span)
        group_pieces.append(ring(jnp.concatenate([w_key[:, cut], w_value[:, cut]], axis=1)))
    own_columns = out_pieces(w_out)

    queries = project_normed(tokens, query_pieces, "queries")
    next_queries = shifted(queries[:block_len], "seq", -1)
    parts = []
    for g in range(groups):
        key_value = project(bank, group_pieces[g], f"keys_values_{g}")
        attended = attend(queries, next_queries, key_value, slots, g * heads, heads, f"attend_{g}")
        for piece, device in every_head(attended):
            parts.append((piece, device * local_width + g * span))
    moved = combine(parts, own_columns, "cross_out")
    first = shifted(moved[tok_rows - block_len :], "seq", 1)
    return jnp.concatenate([first, moved[: tok_rows - block_len]], axis=0)


def solution(mesh):
    in_specs = (
        P(("batch", "seq"), None),
        P(("batch", "seq"), None, None),
        P(("batch", "seq")),
        P("seq", "head"),
        P("seq", "head"),
        P("seq", "head"),
        P("head", "seq"),
    )
    out_specs = P(("batch", "seq"), "head")
    return jax.shard_map(local, mesh=mesh, in_specs=in_specs, out_specs=out_specs, check_vma=False)
```
